8 devices in a mesh: rep: 1 (over z), dp: 8 (over x, y, core).
Axes of the slice: x: 2, y: 2, z: 1, core: 2. Of those that a mesh axis runs over, the one named last changes fastest.
Arguments:
- x: bfloat16 [8, 2048, 1280], P(('rep', 'dp'))
- dy: bfloat16 [8, 2048, 1280], P(('rep', 'dp'))
- w_gate: bfloat16 [2, 1280, 4480], P(None, 'dp')
- w_up: bfloat16 [2, 1280, 4480], P(None, 'dp')
- w_down: bfloat16 [2, 4480, 1280], P(None, 'dp')
Outputs:
- output 1: bfloat16 [8, 2048, 1280], P(('rep', 'dp'))
- output 2: bfloat16 [2, 1280, 4480], P('rep', 'dp')
- output 3: bfloat16 [2, 1280, 4480], P('rep', 'dp')
- output 4: bfloat16 [2, 4480, 1280], P('rep', 'dp')
All inputs are finite; a program needn't handle non-finite values.
Results may differ from the reference program's by a relative error of at most 0.018.
Values are sent between devices in bfloat16 or wider.
A program may use at most 2 GiB of HBM per device.

```python
import jax
import jax.numpy as jnp
from jax import lax

SEQUENCES = 8
TOKENS = 2048
D = 1280
FF = 4480
LAYERS = 2
NAMES = ("w_gate", "w_up", "w_down")
SHAPES = {"w_gate": (LAYERS, D, FF), "w_up": (LAYERS, D, FF), "w_down": (LAYERS, FF, D)}


def bump(key, n, height):
    away = (jnp.arange(n, dtype=jnp.int32) - jax.random.randint(key, (), 0, n, jnp.int32)) % n
    return jnp.where(away < n // 8, height, 1.0)


def together(key, own, strength):
    shared = jax.random.normal(key, own.shape[1:], jnp.float32)
    return (own + strength * shared) * lax.rsqrt(1 + strength * strength)


def setup_inputs(seed: int = 0, part: int = 0) -> dict:
    kx, kdy, ka, kb, kz, kf, kh, kl, *kw = jax.random.split(jax.random.key(seed), 8 + len(NAMES))
    kx, kdy, ka, kb = (jax.random.fold_in(k, part) for k in (kx, kdy, ka, kb))
    shape = (SEQUENCES, TOKENS, D)
    much_x, much_dy = jax.random.uniform(kz, (2,), jnp.float32, 0.0, 1.0)
    layers = 2.0 ** jax.random.uniform(kl, (LAYERS, 1, 1), jnp.float32, -1.0, 1.0)
    x = together(ka, jax.random.normal(kx, shape, jnp.float32), much_x) * bump(kf, D, 4.0)
    dy = together(kb, jax.random.normal(kdy, shape, jnp.float32), much_dy)
    drawn = {"x": x.astype(jnp.bfloat16), "dy": (dy * (SEQUENCES * TOKENS) ** -0.5).astype(jnp.bfloat16)}
    for key, name in zip(kw, NAMES, strict=True):
        w = jax.random.normal(key, SHAPES[name], jnp.float32) * SHAPES[name][1] ** -0.5
        drawn[name] = (w * {"w_gate": 1.0, "w_up": bump(kh, FF, 4.0), "w_down": layers}[name]).astype(jnp.bfloat16)
    return drawn


def matmul(a, w):
    return jnp.dot(a, w, preferred_element_type=jnp.float32).astype(jnp.bfloat16)


def normed(h):
    wide = h.astype(jnp.float32)
    scale = lax.rsqrt(jnp.mean(wide**2, -1, keepdims=True) + 1e-6)
    return (wide * scale).astype(jnp.bfloat16)


def layer(h, w):
    a = normed(h)
    gate = jnp.dot(a, w["w_gate"], preferred_element_type=jnp.float32)
    up = jnp.dot(a, w["w_up"], preferred_element_type=jnp.float32)
    return h + matmul((jax.nn.silu(gate) * up).astype(jnp.bfloat16), w["w_down"])


def stack(weights, h):
    return lax.scan(lambda h, w: (layer(h, w), None), h, weights)[0]


def reference(x, dy, w_gate, w_up, w_down):
    weights = dict(zip(NAMES, (w_gate, w_up, w_down), strict=True))

    def take(so_far, sequence):
        h, by_y = sequence
        _, back = jax.vjp(stack, weights, h)
        by_weights, by_h = back(by_y)
        return jax.tree.map(lambda total, term: total + term.astype(jnp.float32), so_far, by_weights), by_h

    none_yet = {name: jnp.zeros(w.shape, jnp.float32) for name, w in weights.items()}
    by_weights, by_x = lax.scan(take, none_yet, (x, dy))
    return (by_x, *(by_weights[name].astype(jnp.bfloat16) for name in NAMES))
```

```python
import jax
import jax.numpy as jnp
from jax import lax
from jax.sharding import PartitionSpec as P

F32, BF16 = jnp.float32, jnp.bfloat16
BOTH = ("rep", "dp")


def dot(a, b, contract):
    return lax.dot_general(a, b, (contract, ((), ())), preferred_element_type=F32)


def gathered(w):
    return lax.all_gather(w, "dp", axis=0, tiled=True)


def scattered(term):
    return lax.psum_scatter(term.astype(BF16), "dp", scatter_dimension=0, tiled=True)


def body(x, dy, w_gate, w_up, w_down):
    layers = w_gate.shape[0]
    h, dh = x[0], dy[0]
    weights, saved = [], []
    for n in range(layers):
        wg, wu, wd = (gathered(w[n]) for w in (w_gate, w_up, w_down))
        weights.append((wg, wu, wd))
        wide = h.astype(F32)
        scale = lax.rsqrt(jnp.mean(wide**2, -1, keepdims=True) + 1e-6)
        a = (wide * scale).astype(BF16)
        gate = dot(a, wg, ((1,), (0,)))
        up = dot(a, wu, ((1,), (0,)))
        z = (jax.nn.silu(gate) * up).astype(BF16)
        saved.append((h, scale, a, gate, up, z))
        if n < layers - 1:
            h = h + dot(z, wd, ((1,), (0,))).astype(BF16)

    grads = []
    for n in reversed(range(layers)):
        wg, wu, wd = weights[n]
        h, scale, a, gate, up, z = saved[n]
        by_down = scattered(dot(z, dh, ((0,), (0,))))
        dz = dot(dh, wd, ((1,), (1,))).astype(BF16).astype(F32)
        s = jax.nn.sigmoid(gate)
        d_up = (dz * (gate * s)).astype(BF16)
        d_gate = (dz * up * (s * (1 + gate * (1 - s)))).astype(BF16)
        by_gate = scattered(dot(a, d_gate, ((0,), (0,))))
        by_up = scattered(dot(a, d_up, ((0,), (0,))))
        da = (dot(d_gate, wg, ((1,), (1,))) + dot(d_up, wu, ((1,), (1,)))).astype(BF16)
        da, wide = da.astype(F32), h.astype(F32)
        inner = jnp.mean(da * wide, -1, keepdims=True)
        dh = dh + (scale * (da - wide * (scale * scale * inner))).astype(BF16)
        grads.append((by_gate, by_up, by_down))

    return (dh[None], *(jnp.stack(g) for g in zip(*reversed(grads), strict=True)))


def solution(mesh):
    seq, shard = P(BOTH, None, None), P(None, "dp", None)
    return jax.shard_map(
        body,
        mesh=mesh,
        in_specs=(seq, seq, shard, shard, shard),
        out_specs=(seq, P("rep", "dp", None), P("rep", "dp", None), P("rep", "dp", None)),
        check_vma=False,
    )
```

```python
import functools

import jax
import jax.numpy as jnp
from jax import lax
from jax.experimental import pallas as pl
from jax.experimental.pallas import tpu as pltpu
from jax.sharding import PartitionSpec as P

F32, BF16 = jnp.float32, jnp.bfloat16
BOTH = ("rep", "dp")
CHIPS = [[0, 2, 4, 6], [1, 3, 5, 7]]
MESH = pl.DeviceIdType.MESH
VMEM_LIMIT = 60 * 1024 * 1024
TILE = 640
WIDE = 512
DEEP = 1024
KINDS = (
    "own x first",
    "own x second",
    "own y first",
    "own y second",
    "on y",
    "on x",
    "own core",
    "core x first",
    "core y second",
    "core x second",
    "core y first",
    "core far",
)


def dot(a, b, contract):
    return lax.dot_general(a, b, (contract, ((), ())), preferred_element_type=F32)


def meet(partner):
    barrier = pltpu.get_barrier_semaphore()
    pl.semaphore_signal(barrier, inc=1, device_id={"dp": partner}, device_id_type=MESH)
    pl.semaphore_wait(barrier, 1)


def to_partner(src, dst, send, recv, partner):
    return pltpu.make_async_remote_copy(src, dst, send, recv, device_id={"dp": partner}, device_id_type=MESH)


def wide_kernel(steps, a_ref, d_ref, s_ref, term, theirs, send, recv):
    j = pl.program_id(0)
    me = lax.axis_index("dp")
    core = me % 2
    partner = me + 1 - 2 * core
    chips, rows = theirs.shape[1], theirs.shape[2]

    def copies(step):
        return [
            to_partner(term.at[step % 2, 2 * c + 1 - core], theirs.at[step, c], send.at[step % 2, c], recv.at[step, c], partner)
            for c in range(chips)
        ]

    @pl.when(j == 0)
    def _():
        meet(partner)

    @pl.when((j >= 2) & (j - 2 < steps))
    def _():
        for copy in copies(j - 2):
            copy.wait_send()

    @pl.when(j < steps)
    def _():
        out = dot(a_ref[...], d_ref[...], ((1,), (0,))).astype(BF16)
        term[j % 2] = out.reshape(2 * chips, rows, out.shape[1])
        for copy in copies(j):
            copy.start()

    @pl.when(j >= 1)
    def _():
        before = jnp.maximum(j - 1, 0)
        for c, copy in enumerate(copies(before)):
            copy.wait_recv()
            mine = term[before % 2, 2 * c + core].astype(F32)
            s_ref[c] = (mine + theirs[before, c].astype(F32)).astype(BF16)

    @pl.when(j == steps)
    def _():
        for copy in copies(steps - 1):
            copy.wait_send()


def wide_term(a, d):
    depth, tokens = a.shape
    ff = d.shape[1]
    steps = pl.cdiv(ff, WIDE)
    rows = depth // 8
    return pl.pallas_call(
        functools.partial(wide_kernel, steps),
        grid=(steps + 1,),
        in_specs=[
            pl.BlockSpec((depth, tokens), lambda j: (0, 0), pipeline_mode=pl.Buffered(1)),
            pl.BlockSpec((tokens, WIDE), lambda j: (0, jnp.minimum(j, steps - 1))),
        ],
        out_specs=pl.BlockSpec((4, rows, WIDE), lambda j: (0, 0, jnp.maximum(j - 1, 0))),
        out_shape=jax.ShapeDtypeStruct((4, rows, ff), BF16),
        scratch_shapes=[
            pltpu.VMEM((2, 8, rows, WIDE), BF16),
            pltpu.VMEM((steps, 4, rows, WIDE), BF16),
            pltpu.SemaphoreType.DMA((2, 4)),
            pltpu.SemaphoreType.DMA((steps, 4)),
        ],
        compiler_params=pltpu.CompilerParams(collective_id=0, has_side_effects=True, vmem_limit_bytes=VMEM_LIMIT),
        cost_estimate=pl.CostEstimate(flops=2 * tokens * depth * ff, bytes_accessed=40 << 20, transcendentals=0),
        name="wide_term",
    )(a, d).reshape(4 * rows, ff)


def tall_kernel(steps, z_ref, d_ref, s_ref, term, theirs, send, recv):
    j = pl.program_id(0)
    me = lax.axis_index("dp")
    core = me % 2
    partner = me + 1 - 2 * core
    chips, rows = theirs.shape[:2]

    def copy(c):
        at = pl.multiple_of((2 * c + 1 - core) * rows, 16)
        return to_partner(term.at[pl.ds(at, rows)], theirs.at[c], send.at[c], recv.at[c], partner)

    @pl.when(j == 0)
    def _():
        meet(partner)

    @pl.when(j < steps)
    def _():
        at = pl.multiple_of(j * TILE, TILE)
        term[pl.ds(at, TILE)] = dot(z_ref[...], d_ref[...], ((0,), (0,))).astype(BF16)

    for c in range(chips):
        whole = -(-(2 * c + 2) * rows // TILE) - 1

        @pl.when(j == whole)
        def _():
            copy(c).start()

    @pl.when(j >= steps)
    def _():
        c = jnp.maximum(j - steps, 0)
        copy(c).wait()
        at = pl.multiple_of((2 * c + core) * rows, 16)
        s_ref[0] = (term[pl.ds(at, rows)].astype(F32) + theirs[c].astype(F32)).astype(BF16)


def tall_term(z, d):
    tokens, ff = z.shape
    depth = d.shape[1]
    steps = ff // TILE
    rows = ff // 8
    return pl.pallas_call(
        functools.partial(tall_kernel, steps),
        grid=(steps + 4,),
        in_specs=[
            pl.BlockSpec((tokens, TILE), lambda j: (0, jnp.minimum(j, steps - 1))),
            pl.BlockSpec((tokens, depth), lambda j: (0, 0), pipeline_mode=pl.Buffered(1)),
        ],
        out_specs=pl.BlockSpec((1, rows, depth), lambda j: (jnp.maximum(j - steps, 0), 0, 0)),
        out_shape=jax.ShapeDtypeStruct((4, rows, depth), BF16),
        scratch_shapes=[
            pltpu.VMEM((ff, depth), BF16),
            pltpu.VMEM((4, rows, depth), BF16),
            pltpu.SemaphoreType.DMA((4,)),
            pltpu.SemaphoreType.DMA((4,)),
        ],
        compiler_params=pltpu.CompilerParams(collective_id=1, has_side_effects=True, vmem_limit_bytes=VMEM_LIMIT),
        cost_estimate=pl.CostEstimate(flops=2 * tokens * depth * ff, bytes_accessed=40 << 20, transcendentals=0),
        name="tall_term",
    )(z, d).reshape(4 * rows, depth)


def forward_kernel(layers, x_ref, *refs):
    count = 3 * layers
    shards, refs = [refs[k].at[n] for n in range(layers) for k in range(3)], refs[3:]
    wholes, refs = refs[:count], refs[count:]
    states, refs = refs[: layers - 1], refs[layers - 1 :]
    normed, gates, by_ups, by_gates, prods, turned = (refs[k * layers :][:layers] for k in range(6))
    refs = refs[6 * layers :]
    a_vm, down_vm, wide_vm, tall_vm, send, recv, local = refs

    me = lax.axis_index("dp")
    cx, cy, core = me // 4, me // 2 % 2, me % 2
    by_x, by_y, partner = me + 4 - 8 * cx, me + 2 - 4 * cy, me + 1 - 2 * core
    far = by_x + by_y - me

    barrier = pltpu.get_barrier_semaphore()
    for other in (by_x, by_y, partner):
        pl.semaphore_signal(barrier, inc=1, device_id={"dp": other}, device_id_type=MESH)
    pl.semaphore_wait(barrier, 3)

    def copy(n, kind):
        shard, whole = shards[n], wholes[n]
        rows = shard.shape[0]
        half = rows // 32 * 16
        first, second, both = (0, half), (half, rows - half), (0, rows)
        whose, (at, size), target = {
            "own x first": (me, first, by_x),
            "own x second": (me, second, by_x),
            "own y first": (me, first, by_y),
            "own y second": (me, second, by_y),
            "on y": (by_x, first, by_y),
            "on x": (by_y, second, by_x),
            "own core": (me, both, partner),
            "core x first": (by_x, first, partner),
            "core y second": (by_y, second, partner),
            "core x second": (by_x, second, partner),
            "core y first": (by_y, first, partner),
            "core far": (far, both, partner),
        }[kind]
        k = KINDS.index(kind)
        place = pl.ds(pl.multiple_of(whose * rows + at, 16), size)
        source = shard.at[pl.ds(at, size)] if kind.startswith("own") else whole.at[place]
        return pltpu.make_async_remote_copy(
            source, whole.at[place], send.at[n, k], recv.at[n, k], device_id={"dp": target}, device_id_type=MESH
        )

    def start(n, *kinds):
        for kind in kinds:
            copy(n, kind).start()

    def arrived(n, *kinds):
        for kind in kinds:
            copy(n, kind).wait_recv()

    def begin(n):
        start(n, "own x first", "own y second", "own x second", "own y first", "own core")

    def hand_on(n):
        arrived(n, "own x first", "own y second")
        start(n, "on y", "on x", "core x first", "core y second")
        if n + 1 < count:
            begin(n + 1)

    def finish(n):
        arrived(n, "own x second", "own y first")
        start(n, "core x second", "core y first")
        arrived(n, "on x", "on y")
        start(n, "core far")
        arrived(n, "own core", *(kind for kind in KINDS if kind.startswith("core")))

    begin(0)
    bounce = []
    for n in range(count):
        buffer = (tall_vm if n % 3 == 2 else wide_vm).at[n // 3 if n % 3 == 2 else n // 3 * 2 + n % 3]
        rows = shards[n].shape[0]
        into = pltpu.make_async_copy(shards[n], buffer, local.at[n])
        out = pltpu.make_async_copy(buffer, wholes[n].at[pl.ds(pl.multiple_of(me * rows, 16), rows)], local.at[n])
        into.start()
        bounce.append((into, out))
    for into, out in bounce:
        into.wait()
        out.start()

    tokens, depth = x_ref.shape
    ff = wholes[0].shape[1]

    def scaled(h):
        wide = h.astype(F32)
        return (wide * lax.rsqrt(jnp.mean(wide**2, -1, keepdims=True) + 1e-6)).astype(BF16)

    def norm_body(h_ref, a_ref, turned_ref):
        a = scaled(h_ref[...])
        a_ref[...] = a
        turned_ref[...] = a.T

    row = lambda width, size=256, first=0: pl.BlockSpec((size, width), lambda j: (j + first, 0))
    column = lambda depth, first=0, size=TILE: pl.BlockSpec((depth, size), lambda j: (0, j + first))

    pltpu.emit_pipeline(norm_body, grid=(tokens // 256,), in_specs=[row(depth)], out_specs=[row(depth), column(depth, 0, 256)])(
        x_ref, normed[0], turned[0]
    )
    for _, out in bounce:
        out.wait()

    def load(src, dst):
        c = pltpu.make_async_copy(src, dst, local.at[0])
        c.start()
        c.wait()

    def gate_body(w_ref, gate_ref):
        @pl.loop(0, tokens // 512)
        def _(r):
            at = pl.ds(r * 512, 512)
            gate_ref[at] = dot(a_vm[at], w_ref[...], ((1,), (0,)))

    def up_body(w_ref, gate_ref, by_up_ref, by_gate_ref, z_ref):
        @pl.loop(0, tokens // 512)
        def _(r):
            at = pl.ds(r * 512, 512)
            up = dot(a_vm[at], w_ref[...], ((1,), (0,)))
            gate = gate_ref[at]
            s = jax.nn.sigmoid(gate)
            by_up = gate * s
            by_up_ref[at] = by_up
            by_gate_ref[at] = up * (s * (1 + gate * (1 - s)))
            z_ref[at] = (by_up * up).astype(BF16)

    def down_body(z_ref, h_ref, next_ref, a_ref, turned_ref):
        h = h_ref[...] + dot(z_ref[...], down_vm[...], ((1,), (0,))).astype(BF16)
        next_ref[...] = h
        a = scaled(h)
        a_ref[...] = a
        turned_ref[...] = a.T

    hand_on(0)
    load(normed[0], a_vm)
    finish(0)
    h = x_ref
    for n in range(layers):
        gate, up, down = 3 * n, 3 * n + 1, 3 * n + 2
        for first, tiles in ((0, 2), (2, ff // TILE - 2)):
            pltpu.emit_pipeline(gate_body, grid=(tiles,), in_specs=[column(depth, first)], out_specs=[column(tokens, first)])(
                wholes[gate], gates[n]
            )
            (hand_on if first == 0 else finish)(up)
        for first, tiles in ((0, 2), (2, ff // TILE - 2)):
            pltpu.emit_pipeline(
                up_body,
                grid=(tiles,),
                in_specs=[column(depth, first), column(tokens, first)],
                out_specs=[column(tokens, first)] * 3,
            )(wholes[up], gates[n], by_ups[n], by_gates[n], prods[n])
            (hand_on if first == 0 else finish)(down)
        if n == layers - 1:
            break
        load(wholes[down], down_vm)
        for first, tiles in ((0, 2), (2, tokens // 256 - 2)):
            pltpu.emit_pipeline(
                down_body,
                grid=(tiles,),
                in_specs=[row(ff, 256, first), row(depth, 256, first)],
                out_specs=[row(depth, 256, first), row(depth, 256, first), column(depth, first, 256)],
            )(prods[n], h, states[n], normed[n + 1], turned[n + 1])
            (hand_on if first == 0 else finish)(3 * n + 3)
        h = states[n]
        load(normed[n + 1], a_vm)

    for n in range(count):
        for kind in KINDS:
            copy(n, kind).wait_send()


def forward(x, *stacked):
    layers = stacked[0].shape[0]
    tokens, depth = x.shape
    shards = [jax.ShapeDtypeStruct(w.shape[1:], w.dtype) for w in stacked] * layers
    ff = shards[0].shape[1]
    array = jax.ShapeDtypeStruct
    shapes = (
        [array((8 * s.shape[0], s.shape[1]), BF16) for s in shards]
        + [array((tokens, depth), BF16)] * (layers - 1)
        + [array((tokens, depth), BF16)] * layers
        + [array((tokens, ff), F32)] * (3 * layers)
        + [array((tokens, ff), BF16)] * layers
        + [array((depth, tokens), BF16)] * layers
    )
    anywhere = pl.BlockSpec(memory_space=pl.ANY)
    out = pl.pallas_call(
        functools.partial(forward_kernel, layers),
        in_specs=[anywhere] * (1 + len(stacked)),
        out_specs=[anywhere] * len(shapes),
        out_shape=shapes,
        scratch_shapes=[
            pltpu.VMEM((tokens, depth), BF16),
            pltpu.VMEM((ff, depth), BF16),
            pltpu.VMEM((2 * layers, *shards[0].shape), BF16),
            pltpu.VMEM((layers, *shards[2].shape), BF16),
            pltpu.SemaphoreType.DMA((len(shards), len(KINDS))),
            pltpu.SemaphoreType.DMA((len(shards), len(KINDS))),
            pltpu.SemaphoreType.DMA((len(shards),)),
        ],
        compiler_params=pltpu.CompilerParams(collective_id=2, has_side_effects=True, vmem_limit_bytes=67043328),
        cost_estimate=pl.CostEstimate(flops=10 * tokens * depth * ff, bytes_accessed=400 << 20, transcendentals=0),
        name="forward",
    )(x, *stacked)
    k = len(shards)
    return out[:k], out[k : k + layers - 1], [out[k + layers - 1 + i * layers :][:layers] for i in range(6)]


def hidden_kernel(dh_ref, down_ref, by_gate_ref, by_up_ref, d_gate_ref, d_up_ref):
    for r in range(dh_ref.shape[0] // 512):
        at = pl.ds(r * 512, 512)
        dz = dot(dh_ref[at], down_ref[...], ((1,), (1,))).astype(BF16).astype(F32)
        d_up_ref[at] = (dz * by_up_ref[at]).astype(BF16)
        d_gate_ref[at] = (dz * by_gate_ref[at]).astype(BF16)


def hidden(dh, down, by_gate, by_up):
    tokens, ff = by_gate.shape
    depth = dh.shape[1]
    column = pl.BlockSpec((tokens, WIDE), lambda j: (0, j))
    return pl.pallas_call(
        hidden_kernel,
        grid=(pl.cdiv(ff, WIDE),),
        in_specs=[
            pl.BlockSpec((tokens, depth), lambda j: (0, 0), pipeline_mode=pl.Buffered(1)),
            pl.BlockSpec((WIDE, depth), lambda j: (j, 0)),
            column,
            column,
        ],
        out_specs=[column, column],
        out_shape=[jax.ShapeDtypeStruct((tokens, ff), BF16)] * 2,
        compiler_params=pltpu.CompilerParams(vmem_limit_bytes=VMEM_LIMIT),
        cost_estimate=pl.CostEstimate(flops=2 * tokens * depth * ff, bytes_accessed=120 << 20, transcendentals=0),
        name="hidden",
    )(dh, down, by_gate, by_up)


def input_kernel(rest, d_gate_ref, d_up_ref, gate_ref, up_ref, h_ref, dh_ref, out_ref, total):
    j = pl.program_id(0)
    last = pl.num_programs(0) - 1

    def term(at, columns):
        return dot(d_gate_ref[at, columns], gate_ref[:, columns], ((1,), (1,))) + dot(d_up_ref[at, columns], up_ref[:, columns], ((1,), (1,)))

    for r in range(h_ref.shape[0] // 512):
        at = slice(r * 512, r * 512 + 512)

        @pl.when(j == 0)
        def _():
            total[at] = term(at, slice(None))

        @pl.when((j > 0) & (j < last))
        def _():
            total[at] += term(at, slice(None))

        @pl.when(j == last)
        def _():
            total[at] += term(at, slice(0, rest))

    @pl.when(j == last)
    def _():
        @pl.loop(0, h_ref.shape[0] // 128)
        def _(r):
            at = pl.ds(r * 128, 128)
            da = total[at].astype(BF16).astype(F32)
            wide = h_ref[at].astype(F32)
            scale = lax.rsqrt(jnp.mean(wide**2, -1, keepdims=True) + 1e-6)
            inner = jnp.mean(da * wide, -1, keepdims=True)
            out_ref[at] = dh_ref[at] + (scale * (da - wide * (scale * scale * inner))).astype(BF16)


def by_input(d_gate, d_up, gate, up, h, dh):
    tokens, depth = h.shape
    ff = d_gate.shape[1]
    once = pl.BlockSpec((tokens, depth), lambda j: (0, 0), pipeline_mode=pl.Buffered(1))
    return pl.pallas_call(
        functools.partial(input_kernel, ff - (pl.cdiv(ff, DEEP) - 1) * DEEP),
        grid=(pl.cdiv(ff, DEEP),),
        in_specs=[pl.BlockSpec((tokens, DEEP), lambda j: (0, j))] * 2 + [pl.BlockSpec((depth, DEEP), lambda j: (0, j))] * 2 + [once] * 2,
        out_specs=pl.BlockSpec((tokens, depth), lambda j: (0, 0), pipeline_mode=pl.Buffered(1)),
        out_shape=jax.ShapeDtypeStruct((tokens, depth), BF16),
        scratch_shapes=[pltpu.VMEM((tokens, depth), F32)],
        compiler_params=pltpu.CompilerParams(vmem_limit_bytes=VMEM_LIMIT),
        cost_estimate=pl.CostEstimate(flops=4 * tokens * depth * ff, bytes_accessed=80 << 20, transcendentals=0),
        name="by_input",
    )(d_gate, d_up, gate, up, h, dh)


def scattered(chip_sum):
    return lax.psum_scatter(chip_sum, "dp", scatter_dimension=0, tiled=True, axis_index_groups=CHIPS)


def after(first, *values):
    return lax.optimization_barrier((first, *values))


def body(x, dy, w_gate, w_up, w_down):
    layers = w_gate.shape[0]
    h, dh = x[0], dy[0]
    weights, states, kept = forward(h, w_gate, w_up, w_down)
    states = (h, *states)

    grads = []
    for n in reversed(range(layers)):
        wg, wu, wd = weights[3 * n : 3 * n + 3]
        h, (_, _, from_up, from_gate, z, turned) = states[n], (k[n] for k in kept)
        by_down, dh = after(tall_term(z, dh), dh)
        d_gate, d_up = hidden(dh, wd, from_gate, from_up)
        by_gate, d_up = after(wide_term(turned, d_gate), d_up)
        by_up, d_up = after(wide_term(turned, d_up), d_up)
        dh = by_input(d_gate, d_up, wg, wu, h, dh)
        sums = {}
        for name, term in (("down", by_down), ("gate", by_gate), ("up", by_up)):
            sums[name] = scattered(term)
        grads.append([sums[name] for name in ("gate", "up", "down")])

    return (dh[None], *(jnp.stack(g) for g in zip(*reversed(grads), strict=True)))


def solution(mesh):
    seq, shard = P(BOTH, None, None), P(None, "dp", None)

    return jax.shard_map(
        body,
        mesh=mesh,
        in_specs=(seq, seq, shard, shard, shard),
        out_specs=(seq, P("rep", "dp", None), P("rep", "dp", None), P("rep", "dp", None)),
        check_vma=False,
    )
```

```python
import functools

import jax
import jax.numpy as jnp
from jax import lax
from jax.experimental import pallas as pl
from jax.experimental.pallas import tpu as pltpu
from jax.sharding import PartitionSpec as P

F32, BF16 = jnp.float32, jnp.bfloat16
BOTH = ("rep", "dp")
CHIPS = [[0, 2, 4, 6], [1, 3, 5, 7]]
MESH = pl.DeviceIdType.MESH
VMEM_LIMIT = 60 * 1024 * 1024
WHOLE_VMEM = 67043328
TILE = 640
WIDE = 512
ROWS = 256
PARTS = (((0, 5), (5, 4)), ((0, 9),))
KINDS = (
    "own x first",
    "own x second",
    "own y first",
    "own y second",
    "on y",
    "on x",
    "own core",
    "core x first",
    "core y second",
    "core x second",
    "core y first",
    "core far",
)


def dot(a, b, contract):
    return lax.dot_general(a, b, (contract, ((), ())), preferred_element_type=F32)


def meet(partner):
    barrier = pltpu.get_barrier_semaphore()
    pl.semaphore_signal(barrier, inc=1, device_id={"dp": partner}, device_id_type=MESH)
    pl.semaphore_wait(barrier, 1)


def to_partner(src, dst, send, recv, partner):
    return pltpu.make_async_remote_copy(src, dst, send, recv, device_id={"dp": partner}, device_id_type=MESH)


def wide_kernel(steps, a_ref, dh_ref, down_ref, by_gate_ref, by_up_ref, d_gate_ref, d_up_ref, s_ref, term, theirs, send, recv):
    j = pl.program_id(0)
    me = lax.axis_index("dp")
    core = me % 2
    partner = me + 1 - 2 * core
    chips, rows = theirs.shape[2], theirs.shape[3]

    def copies(step):
        return [
            to_partner(
                term.at[step % 2, m, 2 * c + 1 - core], theirs.at[step % 3, m, c], send.at[step % 2, m, c], recv.at[step % 3, m, c], partner
            )
            for m in range(2)
            for c in range(chips)
        ]

    def add():
        for m in range(2):
            for c in range(chips):
                mine = term[(j + 1) % 2, m, 2 * c + core].astype(F32)
                s_ref[c, m] = (mine + theirs[(j + 2) % 3, m, c].astype(F32)).astype(BF16)

    @pl.when(j == 0)
    def _():
        meet(partner)

    @pl.when(j >= 2)
    def _():
        for copy in copies(j - 2):
            copy.wait_send()

    def earlier():
        @pl.when(j >= 1)
        def _():
            for copy in copies(j - 1):
                copy.wait_recv()

        add()

    @pl.when(j < steps)
    def _():
        for r in range(dh_ref.shape[0] // 512):
            at = slice(r * 512, r * 512 + 512)
            dz = dot(dh_ref[at], down_ref[...], ((1,), (1,))).astype(BF16).astype(F32)
            d_up_ref[at] = (dz * by_up_ref[at]).astype(BF16)
            d_gate_ref[at] = (dz * by_gate_ref[at]).astype(BF16)
        for m, d_ref in enumerate((d_gate_ref, d_up_ref)):
            out = dot(a_ref[...], d_ref[...], ((1,), (0,))).astype(BF16)
            term[j % 2, m] = out.reshape(2 * chips, rows, out.shape[1])
            if m == 0:
                earlier()
            for copy in copies(j)[m * chips : m * chips + chips]:
                copy.start()

    @pl.when(j == steps)
    def _():
        earlier()
        for copy in copies(steps - 1):
            copy.wait_send()


def wide_terms(a, dh, down, by_gate, by_up, first, steps):
    depth, tokens = a.shape
    ff = min(by_gate.shape[1] - first * WIDE, steps * WIDE)
    rows = depth // 8
    tile = lambda j: jnp.minimum(j, steps - 1)
    once = lambda *shape: pl.BlockSpec(shape, lambda j: (0, 0), pipeline_mode=pl.Buffered(1))
    column = pl.BlockSpec((tokens, WIDE), lambda j: (0, tile(j)))
    taken = pl.BlockSpec((tokens, WIDE), lambda j: (0, tile(j) + first))
    d_gate, d_up, sums = pl.pallas_call(
        functools.partial(wide_kernel, steps),
        grid=(steps + 1,),
        in_specs=[once(depth, tokens), once(tokens, depth), pl.BlockSpec((WIDE, depth), lambda j: (tile(j) + first, 0)), taken, taken],
        out_specs=[column, column, pl.BlockSpec((4, 2, rows, WIDE), lambda j: (0, 0, 0, jnp.maximum(j - 1, 0)))],
        out_shape=[jax.ShapeDtypeStruct((tokens, ff), BF16)] * 2 + [jax.ShapeDtypeStruct((4, 2, rows, ff), BF16)],
        scratch_shapes=[
            pltpu.VMEM((2, 2, 8, rows, WIDE), BF16),
            pltpu.VMEM((3, 2, 4, rows, WIDE), BF16),
            pltpu.SemaphoreType.DMA((2, 2, 4)),
            pltpu.SemaphoreType.DMA((3, 2, 4)),
        ],
        compiler_params=pltpu.CompilerParams(
            collective_id=4 + 16 * first + steps, has_side_effects=True, vmem_limit_bytes=WHOLE_VMEM
        ),
        cost_estimate=pl.CostEstimate(flops=6 * tokens * depth * ff, bytes_accessed=140 << 20, transcendentals=0),
        name="wide_terms",
    )(a, dh, down, by_gate, by_up)
    return d_gate, d_up, sums.reshape(8 * rows, ff)


def tall_kernel(steps, z_ref, d_ref, s_ref, term, theirs, send, recv):
    j = pl.program_id(0)
    me = lax.axis_index("dp")
    core = me % 2
    partner = me + 1 - 2 * core
    chips, rows = theirs.shape[:2]

    def copy(c):
        at = pl.multiple_of((2 * c + 1 - core) * rows, 16)
        return to_partner(term.at[pl.ds(at, rows)], theirs.at[c], send.at[c], recv.at[c], partner)

    @pl.when(j == 0)
    def _():
        meet(partner)

    @pl.when(j < steps)
    def _():
        at = pl.multiple_of(j * TILE, TILE)
        term[pl.ds(at, TILE)] = dot(z_ref[...], d_ref[...], ((0,), (0,))).astype(BF16)

    for c in range(chips):
        whole = -(-(2 * c + 2) * rows // TILE) - 1

        @pl.when(j == whole)
        def _():
            copy(c).start()

    @pl.when((j >= 2) & (j % 2 == 0) | (j == steps))
    def _():
        c = jnp.maximum(j - 1, 0) // 2
        copy(c).wait()
        at = pl.multiple_of((2 * c + core) * rows, 16)
        s_ref[0] = (term[pl.ds(at, rows)].astype(F32) + theirs[c].astype(F32)).astype(BF16)


def tall_term(z, d):
    tokens, ff = z.shape
    depth = d.shape[1]
    steps = ff // TILE
    rows = ff // 8
    return pl.pallas_call(
        functools.partial(tall_kernel, steps),
        grid=(steps + 1,),
        in_specs=[
            pl.BlockSpec((tokens, TILE), lambda j: (0, jnp.minimum(j, steps - 1))),
            pl.BlockSpec((tokens, depth), lambda j: (0, 0), pipeline_mode=pl.Buffered(1)),
        ],
        out_specs=pl.BlockSpec((1, rows, depth), lambda j: (jnp.maximum(j - 1, 0) // 2, 0, 0)),
        out_shape=jax.ShapeDtypeStruct((4, rows, depth), BF16),
        scratch_shapes=[
            pltpu.VMEM((ff, depth), BF16),
            pltpu.VMEM((4, rows, depth), BF16),
            pltpu.SemaphoreType.DMA((4,)),
            pltpu.SemaphoreType.DMA((4,)),
        ],
        compiler_params=pltpu.CompilerParams(collective_id=1, has_side_effects=True, vmem_limit_bytes=VMEM_LIMIT),
        cost_estimate=pl.CostEstimate(flops=2 * tokens * depth * ff, bytes_accessed=40 << 20, transcendentals=0),
        name="tall_term",
    )(z, d).reshape(4 * rows, depth)


def forward_kernel(layers, x_ref, *refs):
    count = 3 * layers
    shards, refs = [refs[k].at[n] for n in range(layers) for k in range(3)], refs[3:]
    wholes, refs = refs[:count], refs[count:]
    states, refs = refs[: layers - 1], refs[layers - 1 :]
    normed, gates, by_ups, by_gates, prods, turned = (refs[k * layers :][:layers] for k in range(6))
    refs = refs[6 * layers :]
    a_vm, down_vm, wide_vm, tall_vm, send, recv, local = refs

    me = lax.axis_index("dp")
    cx, cy, core = me // 4, me // 2 % 2, me % 2
    by_x, by_y, partner = me + 4 - 8 * cx, me + 2 - 4 * cy, me + 1 - 2 * core
    far = by_x + by_y - me

    barrier = pltpu.get_barrier_semaphore()
    for other in (by_x, by_y, partner):
        pl.semaphore_signal(barrier, inc=1, device_id={"dp": other}, device_id_type=MESH)
    pl.semaphore_wait(barrier, 3)

    def copy(n, kind):
        shard, whole = shards[n], wholes[n]
        rows = shard.shape[0]
        half = rows // 32 * 16
        first, second, both = (0, half), (half, rows - half), (0, rows)
        whose, (at, size), target = {
            "own x first": (me, first, by_x),
            "own x second": (me, second, by_x),
            "own y first": (me, first, by_y),
            "own y second": (me, second, by_y),
            "on y": (by_x, first, by_y),
            "on x": (by_y, second, by_x),
            "own core": (me, both, partner),
            "core x first": (by_x, first, partner),
            "core y second": (by_y, second, partner),
            "core x second": (by_x, second, partner),
            "core y first": (by_y, first, partner),
            "core far": (far, both, partner),
        }[kind]
        k = KINDS.index(kind)
        place = pl.ds(pl.multiple_of(whose * rows + at, 16), size)
        source = shard.at[pl.ds(at, size)] if kind.startswith("own") else whole.at[place]
        return pltpu.make_async_remote_copy(
            source, whole.at[place], send.at[n, k], recv.at[n, k], device_id={"dp": target}, device_id_type=MESH
        )

    def start(n, *kinds):
        for kind in kinds:
            copy(n, kind).start()

    def arrived(n, *kinds):
        for kind in kinds:
            copy(n, kind).wait_recv()

    def begin(n):
        start(n, "own x first", "own y second", "own x second", "own y first", "own core")

    def hand_on(n):
        arrived(n, "own x first", "own y second")
        start(n, "on y", "on x", "core x first", "core y second")
        if n + 1 < count:
            begin(n + 1)

    def finish(n):
        arrived(n, "own x second", "own y first")
        start(n, "core x second", "core y first")
        arrived(n, "on x", "on y")
        start(n, "core far")
        arrived(n, "own core", *(kind for kind in KINDS if kind.startswith("core")))

    begin(0)
    bounce = []
    for n in range(count):
        buffer = (tall_vm if n % 3 == 2 else wide_vm).at[n // 3 if n % 3 == 2 else n // 3 * 2 + n % 3]
        rows = shards[n].shape[0]
        into = pltpu.make_async_copy(shards[n], buffer, local.at[n])
        out = pltpu.make_async_copy(buffer, wholes[n].at[pl.ds(pl.multiple_of(me * rows, 16), rows)], local.at[n])
        into.start()
        bounce.append((into, out))
    for into, out in bounce:
        into.wait()
        out.start()

    tokens, depth = x_ref.shape
    ff = wholes[0].shape[1]

    def scaled(h):
        wide = h.astype(F32)
        return (wide * lax.rsqrt(jnp.mean(wide**2, -1, keepdims=True) + 1e-6)).astype(BF16)

    def norm_body(h_ref, a_ref, turned_ref):
        a = scaled(h_ref[...])
        a_ref[...] = a
        turned_ref[...] = a.T

    row = lambda width, size=256, first=0: pl.BlockSpec((size, width), lambda j: (j + first, 0))
    column = lambda depth, first=0, size=TILE: pl.BlockSpec((depth, size), lambda j: (0, j + first))

    pltpu.emit_pipeline(norm_body, grid=(tokens // 256,), in_specs=[row(depth)], out_specs=[row(depth), column(depth, 0, 256)])(
        x_ref, normed[0], turned[0]
    )
    for _, out in bounce:
        out.wait()

    def load(src, dst):
        c = pltpu.make_async_copy(src, dst, local.at[0])
        c.start()
        c.wait()

    def gate_body(w_ref, gate_ref):
        for r in range(tokens // 512):
            at = pl.ds(r * 512, 512)
            gate_ref[at] = dot(a_vm[at], w_ref[...], ((1,), (0,)))

    def up_body(w_ref, gate_ref, by_up_ref, by_gate_ref, z_ref):
        for r in range(tokens // 512):
            at = pl.ds(r * 512, 512)
            up = dot(a_vm[at], w_ref[...], ((1,), (0,)))
            gate = gate_ref[at]
            s = jax.nn.sigmoid(gate)
            by_up = gate * s
            by_up_ref[at] = by_up
            by_gate_ref[at] = up * (s * (1 + gate * (1 - s)))
            z_ref[at] = (by_up * up).astype(BF16)

    def down_body(z_ref, h_ref, next_ref, a_ref, turned_ref):
        h = h_ref[...] + dot(z_ref[...], down_vm[...], ((1,), (0,))).astype(BF16)
        next_ref[...] = h
        a = scaled(h)
        a_ref[...] = a
        turned_ref[...] = a.T

    hand_on(0)
    load(normed[0], a_vm)
    finish(0)
    h = x_ref
    for n in range(layers):
        gate, up, down = 3 * n, 3 * n + 1, 3 * n + 2
        for first, tiles in ((0, 2), (2, ff // TILE - 2)):
            pltpu.emit_pipeline(gate_body, grid=(tiles,), in_specs=[column(depth, first)], out_specs=[column(tokens, first)])(
                wholes[gate], gates[n]
            )
            (hand_on if first == 0 else finish)(up)
        for first, tiles in ((0, 2), (2, ff // TILE - 2)):
            pltpu.emit_pipeline(
                up_body,
                grid=(tiles,),
                in_specs=[column(depth, first), column(tokens, first)],
                out_specs=[column(tokens, first)] * 3,
            )(wholes[up], gates[n], by_ups[n], by_gates[n], prods[n])
            (hand_on if first == 0 else finish)(down)
        if n == layers - 1:
            break
        load(wholes[down], down_vm)
        for first, tiles in ((0, 2), (2, tokens // 256 - 2)):
            pltpu.emit_pipeline(
                down_body,
                grid=(tiles,),
                in_specs=[row(ff, 256, first), row(depth, 256, first)],
                out_specs=[row(depth, 256, first), row(depth, 256, first), column(depth, first, 256)],
            )(prods[n], h, states[n], normed[n + 1], turned[n + 1])
            (hand_on if first == 0 else finish)(3 * n + 3)
        h = states[n]
        load(normed[n + 1], a_vm)

    for n in range(count):
        for kind in KINDS:
            copy(n, kind).wait_send()


def forward(x, *stacked):
    layers = stacked[0].shape[0]
    tokens, depth = x.shape
    shards = [jax.ShapeDtypeStruct(w.shape[1:], w.dtype) for w in stacked] * layers
    ff = shards[0].shape[1]
    array = jax.ShapeDtypeStruct
    shapes = (
        [array((8 * s.shape[0], s.shape[1]), BF16) for s in shards]
        + [array((tokens, depth), BF16)] * (layers - 1)
        + [array((tokens, depth), BF16)] * layers
        + [array((tokens, ff), F32)] * (3 * layers)
        + [array((tokens, ff), BF16)] * layers
        + [array((depth, tokens), BF16)] * layers
    )
    anywhere = pl.BlockSpec(memory_space=pl.ANY)
    out = pl.pallas_call(
        functools.partial(forward_kernel, layers),
        in_specs=[anywhere] * (1 + len(stacked)),
        out_specs=[anywhere] * len(shapes),
        out_shape=shapes,
        scratch_shapes=[
            pltpu.VMEM((tokens, depth), BF16),
            pltpu.VMEM((ff, depth), BF16),
            pltpu.VMEM((2 * layers, *shards[0].shape), BF16),
            pltpu.VMEM((layers, *shards[2].shape), BF16),
            pltpu.SemaphoreType.DMA((len(shards), len(KINDS))),
            pltpu.SemaphoreType.DMA((len(shards), len(KINDS))),
            pltpu.SemaphoreType.DMA((len(shards),)),
        ],
        compiler_params=pltpu.CompilerParams(collective_id=2, has_side_effects=True, vmem_limit_bytes=WHOLE_VMEM),
        cost_estimate=pl.CostEstimate(flops=10 * tokens * depth * ff, bytes_accessed=400 << 20, transcendentals=0),
        name="forward",
    )(x, *stacked)
    k = len(shards)
    return out[:k], out[k : k + layers - 1], [out[k + layers - 1 + i * layers :][:layers] for i in range(6)]


def input_kernel(*refs):
    *d_refs, gate_ref, up_ref, h_ref, dh_ref, out_ref = refs
    da, at = 0.0, 0
    for d_gate_ref, d_up_ref in zip(d_refs[::2], d_refs[1::2]):
        columns = slice(at, at + d_gate_ref.shape[1])
        da += dot(d_gate_ref[...], gate_ref[:, columns], ((1,), (1,))) + dot(d_up_ref[...], up_ref[:, columns], ((1,), (1,)))
        at = columns.stop
    da = da.astype(BF16).astype(F32)
    wide = h_ref[...].astype(F32)
    scale = lax.rsqrt(jnp.mean(wide**2, -1, keepdims=True) + 1e-6)
    inner = jnp.mean(da * wide, -1, keepdims=True)
    out_ref[...] = dh_ref[...] + (scale * (da - wide * (scale * scale * inner))).astype(BF16)


def by_input(parts, gate, up, h, dh):
    tokens, depth = h.shape
    ff = gate.shape[1]
    row = lambda width: pl.BlockSpec((ROWS, width), lambda j: (j, 0))
    whole = pl.BlockSpec((depth, ff), lambda j: (0, 0), pipeline_mode=pl.Buffered(1))
    return pl.pallas_call(
        input_kernel,
        grid=(tokens // ROWS,),
        in_specs=[*(row(d.shape[1]) for d in parts), whole, whole, row(depth), row(depth)],
        out_specs=row(depth),
        out_shape=jax.ShapeDtypeStruct((tokens, depth), BF16),
        compiler_params=pltpu.CompilerParams(vmem_limit_bytes=VMEM_LIMIT),
        cost_estimate=pl.CostEstimate(flops=4 * tokens * depth * ff, bytes_accessed=80 << 20, transcendentals=0),
        name="by_input",
    )(*parts, gate, up, h, dh)


def scattered(chip_sum):
    return lax.psum_scatter(chip_sum, "dp", scatter_dimension=0, tiled=True, axis_index_groups=CHIPS)


def after(first, *values):
    return lax.optimization_barrier((first, *values))


def body(x, dy, w_gate, w_up, w_down):
    layers = w_gate.shape[0]
    h, dh = x[0], dy[0]
    weights, states, kept = forward(h, w_gate, w_up, w_down)
    states = (h, *states)

    grads = []
    for n in reversed(range(layers)):
        wg, wu, wd = weights[3 * n : 3 * n + 3]
        h, (_, _, from_up, from_gate, z, turned) = states[n], (k[n] for k in kept)
        by_down, dh = after(tall_term(z, dh), dh)
        by_down = scattered(by_down)
        parts, by_wide, d = [], [], dh
        for first, steps in PARTS[n]:
            d_gate, d_up, sums = wide_terms(turned, d, wd, from_gate, from_up, first, steps)
            sums, d = after(sums, d)
            parts += [d_gate, d_up]
            by_wide.append(scattered(sums))
        dh = by_input(parts, wg, wu, h, dh)
        by_wide = jnp.concatenate(by_wide, 1)
        grads.append([*jnp.split(by_wide, 2), by_down])

    return (dh[None], *(jnp.stack(g) for g in zip(*reversed(grads), strict=True)))


def solution(mesh):
    seq, shard = P(BOTH, None, None), P(None, "dp", None)

    return jax.shard_map(
        body,
        mesh=mesh,
        in_specs=(seq, seq, shard, shard, shard),
        out_specs=(seq, P("rep", "dp", None), P("rep", "dp", None), P("rep", "dp", None)),
        check_vma=False,
    )
```
